256 devices in a mesh: cp: 64 (over z, y, core), grp: 4 (over x).
Axes of the slice: x: 4, y: 4, z: 8, core: 2. Of those that a mesh axis runs over, the one named last changes fastest.
Arguments:
- queries: bfloat16 [32768, 4096], P('cp', 'grp'), parts along dimension 1, may hold values from -22.5 to 22.5
- keys: bfloat16 [32768, 512], P('cp', 'grp'), parts along dimension 1, may hold values from -7.5 to 7.5
- values: bfloat16 [32768, 512], P('cp', 'grp'), parts along dimension 1, may hold values from -6 to 6
- grad_out: bfloat16 [32768, 4096], P('cp', 'grp'), parts along dimension 1, may hold values from -6 to 6
- segments: int32 [32768], P('cp'), may hold values from 0 to 127, never falling along the last dimension, each value on 1 to 1025 neighbouring positions
Outputs:
- attended: bfloat16 [32768, 4096], P('cp', 'grp'), parts along dimension 1
- grad_queries: bfloat16 [32768, 4096], P('cp', 'grp'), parts along dimension 1
- grad_keys: bfloat16 [32768, 512], P('cp', 'grp'), parts along dimension 1
- grad_values: bfloat16 [32768, 512], P('cp', 'grp'), parts along dimension 1
The draws below stay inside these ranges and needn't reach their ends.
There are 4 independent parts, one for each index of `grp`. The reference program is written for one: setup_inputs(seed, part) draws one part's arguments, and reference() takes and returns one part's arrays. A program takes and returns all parts, laid end to end along the dimension named above; an argument that names none is the same for every part. Nothing has to cross between parts.
All inputs are finite; a program needn't handle non-finite values.
Results may differ from the reference program's by a relative error of at most 0.028.
Values may be sent and summed in bfloat16 or wider, within the bound.
No kernel may reach another device: no remote copies, remote signals or barrier semaphores. Data moves between devices by JAX's collectives and lax.ppermute only.
A program may use at most 128 MiB of HBM per device.

```python
import math
import jax
import jax.numpy as jnp
import numpy as np
from jax import lax

HEADS = 8
HEAD_DIM = 128
TOK_DEV = 512
REACH = 2
TOKENS = 32768
DOCS = 128
DOC_MOST = 1025


def draw_keys(key, part):
    drawn = jnp.clip(jax.random.normal(jax.random.fold_in(key, 7002), (TOKENS, HEAD_DIM), jnp.float32), -4.0, 4.0)
    return drawn.astype(jnp.bfloat16)


def draw_queries(key, part):
    drawn = jnp.clip(jax.random.normal(jax.random.fold_in(key, 7003), (TOKENS, HEADS * HEAD_DIM), jnp.float32), -4.0, 4.0)
    return drawn.astype(jnp.bfloat16)


def level_of(key, dims, split, smallest, largest):
    def one(dim, blocks):
        steps = jax.random.uniform(jax.random.fold_in(jax.random.fold_in(key, 6), dim), (blocks,), jnp.float32, smallest / len(split), largest / len(split))
        return jnp.repeat(jnp.exp(steps), dims[dim] // blocks).reshape((-1,) + (1,) * (len(dims) - dim - 1))

    level = one(*split[0])
    for cut in split[1:]:
        level = level * one(*cut)
    return level


def profile(number_of, total, most, lean):
    loads = [(1 << 20) // math.isqrt(grade ** lean) + 1 for grade in range(2, number_of + 1)]
    rest, counts = total - most - (number_of - 1), [1] * (number_of - 1)
    while rest > 0:
        free = [i for i in range(number_of - 1) if counts[i] < most]
        pool, left = sum([loads[i] for i in free]), rest
        for i in free:
            more = min(most - counts[i], max(1, left * loads[i] // pool), rest)
            counts[i] = counts[i] + more
            rest = rest - more
    return np.array([most] + counts)


def ragged(stream_key, amount, total, bound, lean):
    if amount == 2:
        one = jax.random.randint(stream_key, (), max(1, total - bound), min(bound, total - 1) + 1)
        return jnp.stack([one, total - one])
    lengths = jnp.asarray(profile(amount, total, bound, lean), jnp.int32)
    twos = (amount - 1) // 2
    source_of, sink = lengths[1:1 + 2 * twos:2], lengths[2:2 + 2 * twos:2]
    room = jnp.minimum(source_of - 1, bound - sink)
    moved = jax.random.randint(jax.random.fold_in(stream_key, 1), (twos,), 0, 1 << 20) % (room + 1)
    lengths = lengths.at[1:1 + 2 * twos:2].set(source_of - moved).at[2:2 + 2 * twos:2].set(sink + moved)
    return lengths[jax.random.permutation(jax.random.fold_in(stream_key, 2), amount)]


def gaussian(own_key, extent, deviation, reach, split=(), held_as=jnp.bfloat16):
    factor_of = level_of(own_key, extent, split, -0.22, 0.18) if split else 1.0
    values = jax.random.normal(own_key, extent, jnp.float32) * deviation * factor_of
    return jnp.minimum(jnp.maximum(values, -reach), reach).astype(held_as)


def setup_inputs(seed: int = 0, part: int = 0) -> dict:
    splits = jax.random.split(jax.random.key(seed), 6)
    own_keys = jax.random.split(jax.random.fold_in(splits[5], part), 6)
    queries = draw_queries(jax.random.fold_in(jax.random.fold_in(splits[5], part), 71), part)
    keys = draw_keys(jax.random.fold_in(jax.random.fold_in(splits[5], part), 71), part)
    values = gaussian(own_keys[2], (TOKENS, HEAD_DIM), 1.0, 6.0, ((0, 64),))
    grad_out = gaussian(own_keys[3], (TOKENS, HEADS * HEAD_DIM), 1.0, 6.0, ((0, 64),))
    segments = jnp.searchsorted(jnp.cumsum(ragged(splits[4], DOCS, TOKENS, DOC_MOST, 2)), jnp.arange(TOKENS), side="right").astype(jnp.int32)
    return {"queries": queries, "keys": keys, "values": values, "grad_out": grad_out, "segments": segments}


NEG = -1e+30

def reference(queries, keys, values, grad_out, segments):
    tiles = TOKENS // TOK_DEV
    scale = 1.0 / math.sqrt(HEAD_DIM)
    pad = REACH * TOK_DEV
    span = (REACH + 1) * TOK_DEV
    keys_pad = jnp.concatenate([jnp.zeros((pad, HEAD_DIM), keys.dtype), keys], axis=0)
    values_pad = jnp.concatenate([jnp.zeros((pad, HEAD_DIM), values.dtype), values], axis=0)
    seg_pad = jnp.concatenate([jnp.full((pad,), -1, jnp.int32), segments.astype(jnp.int32)], axis=0)
    hp = lax.Precision.HIGHEST

    def per_tile(index):
        start = (index * TOK_DEV).astype(jnp.int32)
        query_tile = lax.dynamic_slice_in_dim(queries, start, TOK_DEV, 0).reshape(TOK_DEV, HEADS, HEAD_DIM).astype(jnp.float32)
        grad_tile = lax.dynamic_slice_in_dim(grad_out, start, TOK_DEV, 0).reshape(TOK_DEV, HEADS, HEAD_DIM).astype(jnp.float32)
        seg_query = lax.dynamic_slice_in_dim(segments.astype(jnp.int32), start, TOK_DEV, 0)
        key_win = lax.dynamic_slice_in_dim(keys_pad, start, span, 0).astype(jnp.float32)
        value_win = lax.dynamic_slice_in_dim(values_pad, start, span, 0).astype(jnp.float32)
        seg_win = lax.dynamic_slice_in_dim(seg_pad, start, span, 0)
        query_pos = start + jnp.arange(TOK_DEV, dtype=jnp.int32)
        key_pos = start - pad + jnp.arange(span, dtype=jnp.int32)
        allowed = (seg_query[:, None] == seg_win[None, :]) & (key_pos[None, :] <= query_pos[:, None])
        scores = jnp.einsum('qhd,kd->hqk', query_tile, key_win, precision=hp) * scale
        masked = jnp.where(allowed[None], scores, NEG)
        peak = lax.optimization_barrier(jnp.max(masked, axis=-1))
        total = lax.optimization_barrier(jnp.sum(jnp.where(allowed[None], jnp.exp(scores - peak[..., None]), 0.0), axis=-1))
        lse = peak + jnp.log(total)
        probs = jnp.where(allowed[None], jnp.exp(scores - lse[..., None]), 0.0)
        probs_low = probs.astype(jnp.bfloat16)
        attended = jnp.einsum('hqk,kd->qhd', probs_low.astype(jnp.float32), value_win, precision=hp).astype(jnp.bfloat16)
        delta = lax.optimization_barrier(jnp.sum(grad_tile * attended.astype(jnp.float32), axis=-1)).T
        dprobs = jnp.einsum('qhd,kd->hqk', grad_tile, value_win, precision=hp)
        dscores = (probs * (dprobs - delta[..., None])).astype(jnp.bfloat16).astype(jnp.float32)
        grad_q = (jnp.einsum('hqk,kd->qhd', dscores, key_win, precision=hp) * scale).astype(jnp.bfloat16)
        grad_k = jnp.einsum('hqk,qhd->kd', dscores, query_tile, precision=hp) * scale
        grad_v = jnp.einsum('hqk,qhd->kd', probs_low.astype(jnp.float32), grad_tile, precision=hp)
        return (attended.reshape(TOK_DEV, HEADS * HEAD_DIM), grad_q.reshape(TOK_DEV, HEADS * HEAD_DIM), grad_k.reshape(REACH + 1, TOK_DEV, HEAD_DIM), grad_v.reshape(REACH + 1, TOK_DEV, HEAD_DIM))
    attended, grad_q, grad_k_win, grad_v_win = lax.map(per_tile, jnp.arange(tiles, dtype=jnp.int32))
    key_total = jnp.zeros((tiles + REACH, TOK_DEV, HEAD_DIM), jnp.float32)
    value_total = jnp.zeros((tiles + REACH, TOK_DEV, HEAD_DIM), jnp.float32)
    for slot in range(REACH + 1):
        key_total = key_total.at[slot:slot + tiles].add(grad_k_win[:, slot])
        value_total = value_total.at[slot:slot + tiles].add(grad_v_win[:, slot])
    grad_keys = key_total[REACH:].reshape(TOKENS, HEAD_DIM).astype(jnp.bfloat16)
    grad_values = value_total[REACH:].reshape(TOKENS, HEAD_DIM).astype(jnp.bfloat16)
    return (attended.reshape(TOKENS, HEADS * HEAD_DIM), grad_q.reshape(TOKENS, HEADS * HEAD_DIM), grad_keys, grad_values)
```

```python
import math

import jax
import jax.numpy as jnp
from jax import lax
from jax.experimental import pallas as pl
from jax.experimental.pallas import tpu as pltpu
from jax.sharding import PartitionSpec as P

REACH = 2
BIG = 1e30
HEAD = 128
KEY_BLOCK = 256
GROUP = 2
MOST = 5
PAD = MOST * KEY_BLOCK - REACH * 512 - HEAD

F32 = jnp.float32
BF16 = jnp.bfloat16


def nt(a, b):
    return lax.dot_general(a, b, (((1,), (1,)), ((), ())), preferred_element_type=F32)


def nn(a, b):
    return lax.dot_general(a, b, (((1,), (0,)), ((), ())), preferred_element_type=F32)


def shifted(value, axis, steps):
    count = lax.axis_size(axis)
    first, last = (max(0, -steps), min(count, count - steps))
    return lax.ppermute(value, axis, [(source, source + steps) for source in range(first, last)])


def bits_of(ids, lane):
    return lax.shift_right_logical(ids, lane & 7) & 1


def key_code(ids, lane):
    bits = bits_of(ids, lane)
    return jnp.where(lane < 8, 1 - bits, jnp.where(lane < 16, bits, 0)).astype(F32)


def query_code(ids, lane):
    bits = bits_of(ids, lane)
    return jnp.where(lane < 8, bits, jnp.where(lane < 16, 1 - bits, 0)).astype(F32) * (-BIG)


def pack_kernel(k, v, seg, msg):
    rows = k.shape[0]
    msg[:rows, :HEAD] = k[...]
    msg[:rows, HEAD:] = v[...]
    msg[rows:, :] = jnp.zeros((16, 2 * HEAD), BF16)
    msg[rows : rows + seg.shape[0], :HEAD] = (seg[...] + 1).astype(F32).astype(BF16)


def prep_kernel(q, seg, qt, qcode, kcode):
    rows, width = q.shape
    lane = lax.broadcasted_iota(jnp.int32, (HEAD, HEAD), 1)
    for b in range(rows // HEAD):
        for h in range(width // HEAD):
            block = q[b * HEAD : (b + 1) * HEAD, h * HEAD : (h + 1) * HEAD]
            qt[b, :, h * HEAD : (h + 1) * HEAD] = block.T
        ids = jnp.broadcast_to(seg[b : b + 1, :], (HEAD, HEAD)).T
        qcode[b * HEAD : (b + 1) * HEAD, :] = query_code(ids, lane).astype(BF16)
        kcode[b * HEAD : (b + 1) * HEAD, :] = key_code(ids, lane).astype(BF16)


def main_kernel(
    segs, q, do, k, v, m1, m2, seg, qt, qcode, kcode,
    att, dq, own, far1, far2,
    kwin, vwin, ebuf, dsbuf, dot, dkt, dvt,
):
    rows, width = q.shape
    heads = width // HEAD
    blocks = rows // HEAD
    scale = 1.0 / math.sqrt(HEAD)
    c = scale * math.log2(math.e)
    base = PAD + REACH * rows

    first = segs[0]
    match = (first + 1).astype(F32)
    near = jnp.sum((m1[rows : rows + 16, :HEAD].astype(F32) == match).astype(F32))
    more = jnp.sum((m2[rows : rows + 16, :HEAD].astype(F32) == match).astype(F32))
    before = (near + more).astype(jnp.int32)

    kwin[:PAD, :] = jnp.zeros((PAD, 2 * HEAD), BF16)
    vwin[:PAD, :] = jnp.zeros((PAD, 2 * HEAD), BF16)
    for dist, part in ((2, m2), (1, m1)):
        lo = base - dist * rows
        kwin[lo : lo + rows, :HEAD] = part[:rows, :HEAD]
        vwin[lo : lo + rows, :HEAD] = part[:rows, HEAD:]
    kwin[base:, :HEAD] = k[...]
    vwin[base:, :HEAD] = v[...]
    kwin[base:, HEAD:] = kcode[...]
    vwin[:, HEAD:] = jnp.ones((base + rows, HEAD), BF16)
    row = lax.broadcasted_iota(jnp.int32, (base, HEAD), 0)
    lane = lax.broadcasted_iota(jnp.int32, (base, HEAD), 1)
    reach = jnp.where(row >= base - before, first, 255)
    kwin[:base, HEAD:] = key_code(reach, lane).astype(BF16)

    dkt[...] = jnp.zeros(dkt.shape, F32)
    dvt[...] = jnp.zeros(dvt.shape, F32)

    seg_all = seg[...]
    tri = lax.broadcasted_iota(jnp.int32, (GROUP * HEAD, HEAD), 1) <= (
        lax.broadcasted_iota(jnp.int32, (GROUP * HEAD, HEAD), 0) & (HEAD - 1)
    )

    def one(b, count):
        r0 = pl.multiple_of(b * HEAD, HEAD)
        span = count * KEY_BLOCK
        lo = pl.multiple_of(base + HEAD + r0 - span, HEAD)
        codes = qcode[pl.ds(r0, HEAD), :]
        for g in range(heads // GROUP):
            mine = range(g * GROUP, (g + 1) * GROUP)
            at = slice(g * GROUP * HEAD, (g + 1) * GROUP * HEAD)
            qg = jnp.concatenate(
                [
                    jnp.concatenate([q[pl.ds(r0, HEAD), h * HEAD : (h + 1) * HEAD], codes], axis=1)
                    for h in mine
                ],
                axis=0,
            )
            s = nt(qg, kwin[pl.ds(lo, span), :])
            s = jnp.concatenate(
                [s[:, : span - HEAD], jnp.where(tri, s[:, span - HEAD :], -BIG)], axis=1
            )
            peak = jnp.max(s, axis=1, keepdims=True) * c
            e = jnp.exp2(s * c - peak).astype(BF16)
            ebuf[at, :span] = e
            o = nn(e, vwin[pl.ds(lo, span), :])
            inv = 1.0 / o[:, HEAD:]
            low = (o[:, :HEAD] * inv).astype(BF16)
            dog = jnp.concatenate(
                [do[pl.ds(r0, HEAD), h * HEAD : (h + 1) * HEAD] for h in mine], axis=0
            )
            dos = (dog.astype(F32) * inv).astype(BF16)
            delta = jnp.sum(dos.astype(F32) * low.astype(F32), axis=1, keepdims=True)
            for i, h in enumerate(mine):
                att[pl.ds(r0, HEAD), h * HEAD : (h + 1) * HEAD] = low[i * HEAD : (i + 1) * HEAD]
                dot[:, h * HEAD : (h + 1) * HEAD] = dos[i * HEAD : (i + 1) * HEAD].T
            dp = nt(dos, vwin[pl.ds(lo, span), :HEAD])
            ds = (ebuf[at, :span].astype(F32) * (dp - delta)).astype(BF16)
            dsbuf[at, :span] = ds
            gq = (nn(ds, kwin[pl.ds(lo, span), :HEAD]) * scale).astype(BF16)
            for i, h in enumerate(mine):
                dq[pl.ds(r0, HEAD), h * HEAD : (h + 1) * HEAD] = gq[i * HEAD : (i + 1) * HEAD]
        slot = MOST * 2 + b - 2 * count
        for t in range(count):
            cols = slice(t * KEY_BLOCK, (t + 1) * KEY_BLOCK)
            gk = nn(qt[b], dsbuf[:, cols])
            gv = nn(dot[...], ebuf[:, cols])
            for i in range(2):
                dkt[slot + 2 * t + i] += gk[:, i * HEAD : (i + 1) * HEAD]
                dvt[slot + 2 * t + i] += gv[:, i * HEAD : (i + 1) * HEAD]

    def step(b, carry):
        ahead = jnp.sum((seg_all < segs[b * HEAD]).astype(F32)).astype(jnp.int32)
        start = jnp.where(ahead == 0, -before, ahead)
        need = ((b + 1) * HEAD - start + KEY_BLOCK - 1) // KEY_BLOCK
        for count in range(1, MOST + 1):

            @pl.when(need == count)
            def _():
                one(b, count)

        return carry

    lax.fori_loop(0, blocks, step, 0)

    lead = PAD // HEAD
    for i in range(blocks):
        far2[0, i] = (dkt[lead + i] * scale).astype(BF16)
        far2[1, i] = dvt[lead + i].astype(BF16)
        far1[0, i] = (dkt[lead + blocks + i] * scale).astype(BF16)
        far1[1, i] = dvt[lead + blocks + i].astype(BF16)
        own[0, i] = dkt[lead + 2 * blocks + i] * scale
        own[1, i] = dvt[lead + 2 * blocks + i]


def final_kernel(own, b1, b2, dk, dv):
    for i in range(own.shape[1]):
        rows = slice(i * HEAD, (i + 1) * HEAD)
        for j, out in enumerate((dk, dv)):
            total = own[j, i] + b1[j, i].astype(F32) + b2[j, i].astype(F32)
            out[rows, :] = total.T.astype(BF16)


def on_device(queries, keys, values, grad_out, segments):
    rows, width = queries.shape
    heads = width // HEAD
    blocks = rows // HEAD
    base = PAD + REACH * rows
    seg = segments.reshape(blocks, HEAD)
    shape = jax.ShapeDtypeStruct

    msg = pl.pallas_call(
        pack_kernel, out_shape=shape((rows + 16, 2 * HEAD), BF16), name="pack"
    )(keys, values, seg)
    m1 = shifted(msg, "cp", 1)
    m2 = shifted(msg, "cp", 2)

    qt, qcode, kcode = pl.pallas_call(
        prep_kernel,
        out_shape=(
            shape((blocks, HEAD, width), BF16),
            shape((rows, HEAD), BF16),
            shape((rows, HEAD), BF16),
        ),
        cost_estimate=pl.CostEstimate(
            flops=200_000_000, transcendentals=0, bytes_accessed=4 * rows * width
        ),
        name="prep",
    )(queries, seg)

    grads = (2, blocks, HEAD, HEAD)
    vmem = pl.BlockSpec(memory_space=pltpu.VMEM)
    att, dq, own, far1, far2 = pl.pallas_call(
        main_kernel,
        out_shape=(
            shape((rows, width), BF16),
            shape((rows, width), BF16),
            shape(grads, F32),
            shape(grads, BF16),
            shape(grads, BF16),
        ),
        in_specs=[pl.BlockSpec(memory_space=pltpu.SMEM)] + [vmem] * 10,
        scratch_shapes=[
            pltpu.VMEM((base + rows, 2 * HEAD), BF16),
            pltpu.VMEM((base + rows, 2 * HEAD), BF16),
            pltpu.VMEM((heads * HEAD, MOST * KEY_BLOCK), BF16),
            pltpu.VMEM((heads * HEAD, MOST * KEY_BLOCK), BF16),
            pltpu.VMEM((HEAD, heads * HEAD), BF16),
            pltpu.VMEM(((base + rows) // HEAD, HEAD, HEAD), F32),
            pltpu.VMEM(((base + rows) // HEAD, HEAD, HEAD), F32),
        ],
        cost_estimate=pl.CostEstimate(
            flops=6_000_000_000, transcendentals=4_000_000, bytes_accessed=8 * rows * width
        ),
        compiler_params=pltpu.CompilerParams(vmem_limit_bytes=56 * 1024 * 1024),
        name="attend",
    )(segments, queries, grad_out, keys, values, m1, m2, seg, qt, qcode, kcode)

    b2 = shifted(far2, "cp", -2)
    b1 = shifted(far1, "cp", -1)
    dk, dv = pl.pallas_call(
        final_kernel,
        out_shape=(shape((rows, HEAD), BF16), shape((rows, HEAD), BF16)),
        name="combine",
    )(own, b1, b2)
    return (att, dq, dk, dv)


def solution(mesh):
    placed = (P("cp", "grp"), P("cp", "grp"), P("cp", "grp"), P("cp", "grp"), P("cp"))
    return jax.shard_map(
        on_device,
        mesh=mesh,
        in_specs=placed,
        out_specs=(P("cp", "grp"), P("cp", "grp"), P("cp", "grp"), P("cp", "grp")),
        check_vma=False,
    )
```
